16 devices in a mesh: rep: 4 (over y, z, core), dp: 4 (over x).
Axes of the slice: x: 4, y: 2, z: 1, core: 2. Of those that a mesh axis runs over, the one named last changes fastest.
The devices are a block of a 4x4x8 slice.
Arguments:
- x: bfloat16 [16, 2048, 896], P(('rep', 'dp')), parts along dimension 0
- dy: bfloat16 [16, 2048, 896], P(('rep', 'dp')), parts along dimension 0
- w_gate: bfloat16 [2, 896, 2560], replicated
- w_up: bfloat16 [2, 896, 2560], replicated
- w_down: bfloat16 [2, 2560, 896], replicated
- m_w_gate: float32 [2, 896, 2560], replicated
- m_w_up: float32 [2, 896, 2560], replicated
- m_w_down: float32 [2, 2560, 896], replicated
- v_w_gate: float32 [2, 896, 2560], replicated
- v_w_up: float32 [2, 896, 2560], replicated
- v_w_down: float32 [2, 2560, 896], replicated
Outputs:
- output 1: bfloat16 [8, 896, 2560], P('rep'), parts along dimension 0
- output 2: bfloat16 [8, 896, 2560], P('rep'), parts along dimension 0
- output 3: bfloat16 [8, 2560, 896], P('rep'), parts along dimension 0
- output 4: float32 [8, 896, 2560], P('rep'), parts along dimension 0
- output 5: float32 [8, 896, 2560], P('rep'), parts along dimension 0
- output 6: float32 [8, 2560, 896], P('rep'), parts along dimension 0
- output 7: float32 [8, 896, 2560], P('rep'), parts along dimension 0
- output 8: float32 [8, 896, 2560], P('rep'), parts along dimension 0
- output 9: float32 [8, 2560, 896], P('rep'), parts along dimension 0
There are 4 independent parts. The reference program is written for one: setup_inputs(seed, part) draws one part's arguments, and reference() takes and returns one part's arrays. A program takes and returns all parts, laid end to end along the dimension named above; an argument that names none is the same for every part.
All inputs are finite; a program needn't handle non-finite values.
Results may differ from the reference program's by a relative error of at most 0.022.
Values are sent between devices in bfloat16 or wider.
A program may use at most 768 MiB of HBM per device.

```python
import jax
import jax.numpy as jnp
from jax import lax

SEQUENCES = 4
TOKENS = 2048
D = 896
FF = 2560
LAYERS = 2
NAMES = ("w_gate", "w_up", "w_down")
SHAPES = {"w_gate": (LAYERS, D, FF), "w_up": (LAYERS, D, FF), "w_down": (LAYERS, FF, D)}


def bump(key, n, height):
    away = (jnp.arange(n, dtype=jnp.int32) - jax.random.randint(key, (), 0, n, jnp.int32)) % n
    return jnp.where(away < n // 8, height, 1.0)


def together(key, own, strength):
    shared = jax.random.normal(key, own.shape[1:], jnp.float32)
    return (own + strength * shared) * lax.rsqrt(1 + strength * strength)


def setup_inputs(seed: int = 0, part: int = 0) -> dict:
    kx, kdy, ka, kb, kz, kf, kh, kl, *keys = jax.random.split(jax.random.key(seed), 8 + 3 * len(NAMES))
    kx, kdy, ka, kb = (jax.random.fold_in(k, part) for k in (kx, kdy, ka, kb))
    kw, km, kv = (keys[i::3] for i in range(3))
    shape = (SEQUENCES, TOKENS, D)
    much_x, much_dy = jax.random.uniform(kz, (2,), jnp.float32, 0.0, 1.0)
    loud = 2.0 ** jax.random.uniform(jax.random.fold_in(kz, 1), (), jnp.float32, -1.0, 2.0)
    layers = 2.0 ** jax.random.uniform(kl, (LAYERS, 1, 1), jnp.float32, -1.0, 1.0)
    x = together(ka, jax.random.normal(kx, shape, jnp.float32), much_x) * bump(kf, D, 4.0)
    dy = together(kb, jax.random.normal(kdy, shape, jnp.float32), much_dy)
    drawn = {"x": x.astype(jnp.bfloat16), "dy": (loud * dy * (SEQUENCES * TOKENS) ** -0.5).astype(jnp.bfloat16)}
    for key, name in zip(kw, NAMES, strict=True):
        w = jax.random.normal(key, SHAPES[name], jnp.float32) * SHAPES[name][1] ** -0.5
        drawn[name] = (w * {"w_gate": 1.0, "w_up": bump(kh, FF, 4.0), "w_down": layers}[name]).astype(jnp.bfloat16)
    for key, name in zip(km, NAMES, strict=True):
        drawn[f"m_{name}"] = 0.1 * jax.random.normal(key, SHAPES[name], jnp.float32)
    for key, name in zip(kv, NAMES, strict=True):
        drawn[f"v_{name}"] = jax.random.uniform(key, SHAPES[name], jnp.float32, 0.005, 0.015)
    return drawn


def matmul(a, w):
    return jnp.dot(a, w, preferred_element_type=jnp.float32).astype(jnp.bfloat16)


def normed(h):
    wide = h.astype(jnp.float32)
    scale = lax.rsqrt(jnp.mean(wide**2, -1, keepdims=True) + 1e-6)
    return (wide * scale).astype(jnp.bfloat16)


def layer(h, w):
    a = normed(h)
    gate = jnp.dot(a, w["w_gate"], preferred_element_type=jnp.float32)
    up = jnp.dot(a, w["w_up"], preferred_element_type=jnp.float32)
    return h + matmul((jax.nn.silu(gate) * up).astype(jnp.bfloat16), w["w_down"])


def adamw(w, m, v, g):
    m = 0.9 * m + 0.1 * g
    v = 0.95 * v + 0.05 * g * g
    step = m * lax.rsqrt(v + 1e-8) + 0.1 * w
    return (w - 0.02 * step).astype(jnp.bfloat16), m, v


def stack(weights, h):
    return lax.scan(lambda h, w: (layer(h, w), None), h, weights)[0]


def reference(x, dy, w_gate, w_up, w_down, m_w_gate, m_w_up, m_w_down, v_w_gate, v_w_up, v_w_down):
    weights = dict(zip(NAMES, (w_gate, w_up, w_down), strict=True))

    def take(so_far, sequence):
        h, by_y = sequence
        _, back = jax.vjp(lambda w: stack(w, h), weights)
        return jax.tree.map(lambda total, term: total + term.astype(jnp.float32), so_far, back(by_y)[0]), None

    none_yet = {name: jnp.zeros(w.shape, jnp.float32) for name, w in weights.items()}
    by_weights, _ = lax.scan(take, none_yet, (x, dy))
    gradients = [by_weights[name].astype(jnp.bfloat16).astype(jnp.float32) for name in NAMES]
    new = [
        adamw(w.astype(jnp.float32), m, v, g)
        for w, m, v, g in zip((w_gate, w_up, w_down), (m_w_gate, m_w_up, m_w_down), (v_w_gate, v_w_up, v_w_down), gradients, strict=True)
    ]
    return tuple(one[which] for which in range(3) for one in new)
```

```python
import jax
import jax.numpy as jnp
from jax import lax
from jax.experimental import pallas as pl
from jax.experimental.pallas import tpu as pltpu
from jax.sharding import PartitionSpec as P


BF, F32 = jnp.bfloat16, jnp.float32
ANY = pl.BlockSpec(memory_space=pl.ANY)
STEPS = 4
LANES = 128
WIDTH = 512
VMEM_LIMIT = 60 * 1024 * 1024


def dot(a, b, ca=1, cb=0):
    return lax.dot_general(a, b, (((ca,), (cb,)), ((), ())), preferred_element_type=F32)


def normed(h):
    wide = h.astype(F32)
    scale = lax.rsqrt(jnp.mean(wide**2, -1, keepdims=True) + 1e-6)
    return (wide * scale).astype(BF)


def params():
    return pltpu.CompilerParams(vmem_limit_bytes=VMEM_LIMIT)


def aligned(index, size):
    return pl.ds(pl.multiple_of(index * size, size & -size), size)


def forward_body(x_hbm, wg_ref, wu_ref, wd_ref, a_hbm, h_hbm, b_hbm, x_ref, a_ref, b_ref, acc, sems):
    step, last = pl.program_id(0), pl.num_programs(0) - 1
    count = sems.shape[1]
    size = x_ref.shape[0] // count
    blocks = [pl.ds(i * size, size) for i in range(count)]
    copies = [
        [pltpu.make_async_copy(src.at[rows], dst.at[rows], sems.at[k, i]) for i, rows in enumerate(blocks)]
        for k, (src, dst) in enumerate(((x_hbm, x_ref), (a_ref, a_hbm), (x_ref, h_hbm), (b_ref, b_hbm)))
    ]

    def tile(first, final):
        if first:
            for copy in copies[0]:
                copy.start()
        for i, rows in enumerate(blocks):
            if first:
                copies[0][i].wait()
                a_ref[rows, :] = normed(x_ref[rows, :])
                copies[1][i].start()
            a = a_ref[rows, :]
            gate = dot(a, wg_ref[0])
            up = dot(a, wu_ref[0])
            hidden = (gate * jax.nn.sigmoid(gate) * up).astype(BF)
            part = dot(hidden, wd_ref[0])
            if not first:
                part = acc[rows, :] + part
            if not final:
                acc[rows, :] = part
            else:
                h = (x_ref[rows, :].astype(F32) + part.astype(BF).astype(F32)).astype(BF)
                x_ref[rows, :] = h
                copies[2][i].start()
                b_ref[rows, :] = normed(h)
                copies[3][i].start()
        if final:
            for some in copies[1:]:
                for copy in some:
                    copy.wait()

    pl.when(step == 0)(lambda: tile(True, False))
    pl.when((step > 0) & (step < last))(lambda: tile(False, False))
    pl.when(step == last)(lambda: tile(False, True))


def forward(number, x, wg, wu, wd, width=512, count=4):
    t, d = x.shape
    ff = wg.shape[2]
    col = pl.BlockSpec((1, d, width), lambda i: (number, 0, i))
    return pl.pallas_call(
        forward_body,
        grid=(ff // width,),
        in_specs=[ANY, col, col, pl.BlockSpec((1, width, d), lambda i: (number, i, 0))],
        out_specs=[ANY] * 3,
        out_shape=[jax.ShapeDtypeStruct((t, d), BF)] * 3,
        scratch_shapes=[pltpu.VMEM((t, d), BF)] * 3 + [pltpu.VMEM((t, d), F32), pltpu.SemaphoreType.DMA((4, count))],
        compiler_params=params(),
        cost_estimate=pl.CostEstimate(flops=6 * t * d * ff, bytes_accessed=6 * d * ff + 8 * t * d, transcendentals=t * ff),
        name="forward",
    )(x, wg, wu, wd)


class Kernel:
    def __init__(self, me):
        self.operands, self.in_specs, self.results, self.out_specs, self.scratch = [], [], [], [], []
        self.aliases, self.bodies = {}, []
        self.me = me

    def take(self, array, spec):
        self.operands.append(array)
        self.in_specs.append(spec)
        return ("in", len(self.operands) - 1)

    def give(self, shape, dtype, spec, fill=None):
        self.results.append(jax.ShapeDtypeStruct(shape, dtype))
        self.out_specs.append(spec)
        if fill is not None:
            self.take(fill, ANY)
            self.aliases[len(self.operands)] = len(self.results) - 1
        return ("out", len(self.results) - 1)

    def hold(self, scratch):
        self.scratch.append(scratch)
        return ("scratch", len(self.scratch) - 1)

    def call(self, cost, after, grid=STEPS):
        for array in after:
            self.take(array, ANY)
        counts = len(self.operands), len(self.results)

        def body(me_ref, *refs):
            refs = {"in": refs[: counts[0]], "out": refs[counts[0] : sum(counts)], "scratch": refs[sum(counts) :]}
            get = lambda key: refs[key[0]][key[1]]
            for one in self.bodies:
                one(me_ref[0], get)

        flops, moved, special = cost
        return pl.pallas_call(
            body,
            grid_spec=pltpu.PrefetchScalarGridSpec(
                num_scalar_prefetch=1, grid=(grid,), in_specs=self.in_specs, out_specs=self.out_specs, scratch_shapes=self.scratch
            ),
            out_shape=self.results,
            input_output_aliases=self.aliases,
            compiler_params=params(),
            cost_estimate=pl.CostEstimate(flops=flops, bytes_accessed=moved, transcendentals=special),
        )(self.me, *self.operands)


def whole(shape):
    return pl.BlockSpec(shape, lambda i, me: (0,) * len(shape))


def add_piece(k, ways, piece, a, dy, wg, wu, wd, kept, right, left):
    number, block, width = piece["layer"], piece["block"], piece["width"]
    t, d = a.shape
    rows, units, half = t // STEPS, width // LANES, d // ways // 2
    row = pl.BlockSpec((rows, d), lambda i, me: (i, 0))
    col = pl.BlockSpec((1, d, width), lambda i, me: (number, 0, block))
    a, dy, wg, wu = k.take(a, row), k.take(dy, row), k.take(wg, col), k.take(wu, col)
    wd = k.take(wd, pl.BlockSpec((1, width, d), lambda i, me: (number, block, 0)))
    (right, first), (left, _) = right, left
    near, far, own = (k.give(s, BF, whole(s)) for s in ((n * units, 3, half, LANES) for n in (1, 1, 2)))
    keep = []
    if kept is not None:
        keep = [k.give((t, wg_ff(k, wg)), BF, pl.BlockSpec((rows, width), lambda i, me: (i, block)), fill) for fill in kept]
    acc = k.hold(pltpu.VMEM((3, d, width), F32))

    def body(me, get):
        step = pl.program_id(0)
        total = get(acc)

        def tile(begin):
            x, g = get(a)[...], get(dy)[...]
            gate = dot(x, get(wg)[0])
            up = dot(x, get(wu)[0])
            dh = dot(g, get(wd)[0], 1, 1).astype(BF).astype(F32)
            sig = jax.nn.sigmoid(gate)
            act = gate * sig
            hidden = (act * up).astype(BF)
            dup = (dh * act).astype(BF)
            dgate = (dh * up * (sig * (1 + gate * (1 - sig)))).astype(BF)
            if keep:
                get(keep[0])[...] = dgate
                get(keep[1])[...] = dup
            for i, (l, r) in enumerate(((x, dgate), (x, dup), (g, hidden))):
                part = dot(l, r, 0, 0)
                total[i] = part if begin else total[i] + part

        pl.when(step == 0)(lambda: tile(True))
        pl.when(step > 0)(lambda: tile(False))

        @pl.when(step == STEPS - 1)
        def _():
            where = {
                (0, 0): (own, 0), (0, 1): (own, units), (1, 0): (near, 0), (1, 1): (right, first + units),
                (2, 0): (right, first), (2, 1): (left, first), (3, 0): (left, first + units), (3, 1): (far, 0),
            }
            for (ahead, part), (ref, base) in where.items():
                owner = lax.rem(me + ahead, ways)
                for i in range(3):
                    value = total[i, aligned(owner * 2 + part, half), :].astype(BF)
                    for u in range(units):
                        get(ref)[base + u, i] = value[:, u * LANES : (u + 1) * LANES]

    k.bodies.append(body)
    piece.update(near=near, far=far, own=own)
    return keep


def wg_ff(k, key):
    return k.operands[key[1]].shape[2]


def add_inward(k, number, h, dy, dgate, dup, wg, wu):
    t, d = h.shape
    ff = wg.shape[2]
    rows = t // STEPS
    row = pl.BlockSpec((rows, d), lambda i, me: (i, 0))
    wide = pl.BlockSpec((rows, ff), lambda i, me: (i, 0))
    weight = pl.BlockSpec((1, d, ff), lambda i, me: (number, 0, 0))
    h, dy, dgate, dup, wg, wu = (k.take(x, s) for x, s in ((h, row), (dy, row), (dgate, wide), (dup, wide), (wg, weight), (wu, weight)))
    out = k.give((t, d), BF, row)

    def body(me, get):
        by_gate = dot(get(dgate)[...], get(wg)[0], 1, 1).astype(BF).astype(F32)
        by_up = dot(get(dup)[...], get(wu)[0], 1, 1).astype(BF).astype(F32)
        da = (by_gate + by_up).astype(BF).astype(F32)
        x = get(h)[...].astype(F32)
        scale = lax.rsqrt(jnp.mean(x**2, -1, keepdims=True) + 1e-6)
        inner = jnp.mean(da * x, -1, keepdims=True)
        by_x = da * scale - x * (inner * scale * scale * scale)
        get(out)[...] = (get(dy)[...].astype(F32) + by_x.astype(BF).astype(F32)).astype(BF)

    k.bodies.append(body)
    return out


def add_stage(k, piece, right, left, base):
    units = piece["width"] // LANES
    each = max(1, units // STEPS)
    half = piece["near"].shape[2]
    at = lambda i: i if units >= STEPS else i * units // STEPS

    def part(array, start):
        assert start % each == 0
        return k.take(array, pl.BlockSpec((each, 3, half, LANES), lambda i, me: (start // each + at(i), 0, 0, 0)))

    def sums(*terms):
        def value(get):
            out = get(terms[0])[...].astype(F32)
            for term in terms[1:]:
                out = out + get(term)[...].astype(F32)
            return out.astype(BF)

        return value

    if piece["stage"] == 1:
        (fl, fr), start = piece["m1"]
        writes = [((right,), base, sums(part(piece["near"], 0), part(fl, start)))]
        writes += [((left,), base, sums(part(piece["far"], 0), part(fr, start)))]
    elif piece["stage"] == 2:
        (fl, fr), start = piece["m1"]
        (l2, r2), start2 = piece["m2"]
        a = sums(part(piece["own"], 0), part(l2, start2), part(fr, start + units))
        b = sums(part(piece["own"], units), part(r2, start2), part(fl, start + units))
        writes = [((right, left), base, a), ((right, left), base + units, b)]
    else:
        (fl, fr), start = piece["m3"]
        a, b = part(fl, start), part(fr, start + units)
        writes = [((right,), base, lambda get: get(a)[...]), ((left,), base, lambda get: get(b)[...])]

    def body(me, get):
        for refs, start, value in writes:
            got = value(get)
            for ref in refs:
                get(ref)[pl.ds(start + at(pl.program_id(0)) * each, each)] = got

    k.bodies.append(body)


def adamw(w, m, v, g):
    m = 0.9 * m + 0.1 * g
    v = 0.95 * v + 0.05 * g * g
    step = m * lax.rsqrt(v + 1e-8) + 0.1 * w
    return (w - 0.02 * step).astype(BF), m, v


def update(me, ways, piece, w, m, v, before, after):
    k = Kernel(me)
    number, block, width = piece["layer"], piece["block"], piece["width"]
    d = w[0].shape[1]
    units, half = width // LANES, d // ways // 2
    steps = units

    def section(array, start, size):
        assert start % size == 0
        return k.take(array, pl.BlockSpec((size, 3, half, LANES), lambda i, me: (start // size, 0, 0, 0)))

    (fl, fr), start = piece["m3"]
    own = section(piece["sum"], start, 2 * units)
    left, right = section(fl, start, 2 * units), section(fr, start, 2 * units)
    (fl, fr), start = piece["m4"]
    oa, ob = section(fl, start, units), section(fr, start, units)
    up = pl.BlockSpec((1, d // steps, width), lambda i, me: (number, i, block))
    down = pl.BlockSpec((1, width // steps, d), lambda i, me: (number, block * steps + i, 0))
    specs = [up, up, down]
    sources = [[k.take(x, s) for x, s in zip(some, specs, strict=True)] for some in (w, m, v)]
    fill = iter(before if before is not None else [None] * 9)
    outs = [[k.give(x.shape, dtype, s, next(fill)) for x, s in zip(w, specs, strict=True)] for dtype in (BF, F32, F32)]
    grads = k.hold(pltpu.VMEM((3, d, width), BF))

    def body(me, get):
        step = pl.program_id(0)
        g_ref = get(grads)

        @pl.when(step == 0)
        def _():
            for ahead, part, ref, base in (
                (0, 0, own, 0), (0, 1, own, units), (1, 0, right, 0), (1, 1, right, units),
                (2, 0, oa, 0), (2, 1, ob, 0), (3, 0, left, 0), (3, 1, left, units),
            ):
                owner = lax.rem(me + ahead, ways)
                for i in range(3):
                    for u in range(units):
                        g_ref[i, aligned(owner * 2 + part, half), u * LANES : (u + 1) * LANES] = get(ref)[base + u, i]

        for i in range(3):
            now = [get(some[i])[0] for some in sources]
            if i < 2:
                g = g_ref[i, aligned(step, now[0].shape[0]), :].astype(F32)
            else:
                g = g_ref[i, :, aligned(step, now[0].shape[0])].astype(F32).T
            for out, value in zip(outs, adamw(now[0].astype(F32), now[1], now[2], g), strict=True):
                get(out[i])[0] = value

    k.bodies.append(body)
    return k.call((60 * d * width, 66 * d * width, 3 * d * width), after, steps)


def solution(mesh):
    ways = mesh.shape["dp"]
    assert ways == 4
    rightward = [(i, (i + 1) % ways) for i in range(ways)]
    leftward = [(i, (i - 1) % ways) for i in range(ways)]

    def whole_step(x, dy, *arrays):
        w, m, v = (arrays[i : i + 3] for i in (0, 3, 6))
        layers, d, ff = w[0].shape
        t = x.shape[1]
        half = d // ways // 2
        me = lax.axis_index("dp").astype(jnp.int32).reshape(1)
        h, by_h = x[0], dy[0]
        kept_h, kept_a = [h], []
        for number in range(layers - 1):
            a, h, b = forward(number, h, *w)
            kept_a.append(a)
            kept_h.append(h)
        kept_a.append(b)

        slots = []
        for number in reversed(range(layers)):
            slots += [dict(layer=number, block=i, width=WIDTH, stage=0) for i in range(ff // WIDTH)]
            if number:
                slots.append(number)
        pieces, after, out, kept = [], [], None, [None, None]
        slot = count = 0
        while slot < len(slots) or any(p["stage"] < 5 for p in pieces):
            job = slots[slot] if slot < len(slots) else None
            k = Kernel(me)
            due = [p for p in pieces if p["stage"] < 5 and p["slot"] + 2 * p["stage"] == slot]
            moving = sorted((p for p in due if p["stage"] < 4), key=lambda p: p["stage"] != 2)
            sizes = ([2 * job["width"] // LANES] if isinstance(job, dict) else []) + [
                (1 + (p["stage"] == 2)) * p["width"] // LANES for p in moving
            ]
            shape = (sum(sizes), 3, half, LANES)
            flops, cost = 0, 1 << 22
            if sizes:
                to_right, to_left = k.give(shape, BF, whole(shape)), k.give(shape, BF, whole(shape))
            base = 0
            if isinstance(job, dict):
                keep = add_piece(k, ways, job, kept_a[job["layer"]], by_h, *w, kept if job["layer"] else None, (to_right, 0), (to_left, 0))
                base = sizes[0]
                flops = 12 * t * d * job["width"]
            elif job is not None:
                by_h_key = add_inward(k, job, kept_h[job], by_h, *kept, w[0], w[1])
                flops = 4 * t * d * ff
            for p in moving:
                add_stage(k, p, to_right, to_left, base)
                p["base"] = base
                base += (1 + (p["stage"] == 2)) * p["width"] // LANES
            if k.bodies:
                count += 1
                got = k.call((flops, cost, 0), after + ([out[0]] if out is not None else []))
                after = [got[0]]
                if sizes:
                    sent = got[to_right[1]], got[to_left[1]]
                    to_next = lax.ppermute(sent[0], "dp", rightward)
                    both = to_next, lax.ppermute(sent[1], "dp", leftward)
                if isinstance(job, dict):
                    job.update({n: got[job[n][1]] for n in ("near", "far", "own")}, slot=slot, stage=1, m1=(both, 0))
                    if job["layer"]:
                        kept = [got[key[1]] for key in keep]
                    pieces.append(job)
                elif job is not None:
                    by_h = got[by_h_key[1]]
                    kept = [None, None]
                for p in moving:
                    p["stage"] += 1
                    p[f"m{p['stage']}"] = (both, p["base"])
                    if p["stage"] == 3:
                        p["sum"] = sent[0]
            for p in due:
                if p["stage"] == 4 and p["slot"] + 8 == slot:
                    count += 1
                    out = update(me, ways, p, w, m, v, out, after if k.bodies else [])
                    p["stage"] = 5
            slot += 1
        return tuple(out)

    return jax.shard_map(
        whole_step,
        mesh=mesh,
        in_specs=(P(("rep", "dp"), None, None),) * 2 + (P(None, None, None),) * 9,
        out_specs=(P("rep", None, None),) * 9,
        check_vma=False,
    )
```

```python
import functools

import jax
import jax.numpy as jnp
from jax import lax
from jax.experimental import pallas as pl
from jax.experimental.pallas import tpu as pltpu
from jax.sharding import PartitionSpec as P


BF, F32 = jnp.bfloat16, jnp.float32
ANY = pl.BlockSpec(memory_space=pl.ANY)
LANES = 128
VMEM_LIMIT = 60 * 1024 * 1024


def dot(a, b, ca=1, cb=0):
    return lax.dot_general(a, b, (((ca,), (cb,)), ((), ())), preferred_element_type=F32)


def normed(h):
    wide = h.astype(F32)
    scale = lax.rsqrt(jnp.mean(wide**2, -1, keepdims=True) + 1e-6)
    return (wide * scale).astype(BF)


def params():
    return pltpu.CompilerParams(vmem_limit_bytes=VMEM_LIMIT)


def aligned(index, size):
    return pl.ds(pl.multiple_of(index * size, size & -size), size)


ROWS = 512
PAIR = 2
STAGES = 4
RELAYS = 6


def step_body(ways, groups, x_hbm, x_ref, dy_hbm, wg_ref, wu_ref, wd_ref, wg2_ref, wu2_ref, wd2_ref, *refs):
    count = 2 * len(groups)
    sums, (got1, got2, mine, saved), got3, refs = refs[:count], refs[count : count + 4], refs[count + 4 : count + 8], refs[count + 8 :]
    xh, a_ref, dy, total, at_ref, dyt, both, hid, stage, rin, rout, tin, tout = refs[:13]
    load_sem, in_sem, mine_sem, rin_sem, tin_sem, out_sem, s1_send, s1_recv, s2_send, s2_recv, s3_send, s3_recv, save_sem = refs[13:]
    t, d = xh.shape
    pieces = got1.shape[0]
    n = pieces // 2
    half, width = got2.shape[3:]
    trips = t // ROWS // PAIR
    s = pl.program_id(0)
    steps = n // 2
    r = s - steps
    j = r - n
    lag = n // 2
    inward = (j >= 0) & (j < n)
    q = jnp.where(j < 0, r, jnp.where(inward, -1, j))
    before = jnp.where(j < 0, r - 1, jnp.where(j == 0, n - 1, jnp.where(j > n, j - 1, -1)))
    computes = (q >= 0) & (q < pieces)
    upper = (j < 0).astype(jnp.int32)
    relay_p = jnp.where(j < 0, r - lag, jnp.where(inward, jnp.where(lax.rem(j, 2) == 1, lag + j // 2, -1), jnp.where(j >= n + lag, j - lag, -1)))
    total_p = jnp.where(
        j < 0, -1, jnp.where(inward, jnp.where(lax.rem(j, 2) == 0, j // 2, -1), jnp.where(j < n + lag, j - lag, jnp.where(j >= 2 * n, j - n, -1)))
    )
    me = lax.axis_index("dp")
    right, left = lax.rem(me + 1, ways), lax.rem(me + ways - 1, ways)

    def rows_of(i):
        return pl.ds(i * ROWS if isinstance(i, int) else pl.multiple_of(i * ROWS, ROWS), ROWS)

    def loads(i):
        return pltpu.make_async_copy(x_hbm.at[rows_of(i)], xh.at[rows_of(i)], load_sem.at[i])

    dy_load = pltpu.make_async_copy(dy_hbm, dy, in_sem)

    def save(p):
        return pltpu.make_async_copy(both.at[lax.rem(p, 2)], saved.at[p], save_sem.at[lax.rem(p, 2)])

    def fetch(p):
        return pltpu.make_async_copy(saved.at[p], both.at[lax.rem(p, 2)], save_sem.at[lax.rem(p, 2)])

    lower_half, upper_half = pl.ds(0, half), pl.ds(half, half)

    def share(ahead, part):
        return aligned(lax.rem(me + ahead, ways) * 2 + part, half)

    def first(p):
        slot = lax.rem(p, STAGES)
        return [
            pltpu.make_async_remote_copy(
                src_ref=stage.at[slot, :, pl.ds(pl.multiple_of((lax.rem(me + ahead, ways) * 2 + 1) * half, half & -half), 2 * half)],
                dst_ref=got1.at[p, way], send_sem=s1_send.at[way, p], recv_sem=s1_recv.at[way, p],
                device_id={"dp": to}, device_id_type=pl.DeviceIdType.MESH,
            )
            for way, (ahead, to) in enumerate(((1, right), (2, left)))
        ]

    def second(p):
        slot = lax.rem(p, RELAYS)
        return [
            pltpu.make_async_remote_copy(
                src_ref=rout.at[slot, way], dst_ref=got2.at[p, way], send_sem=s2_send.at[way, p],
                recv_sem=s2_recv.at[way, p], device_id={"dp": to}, device_id_type=pl.DeviceIdType.MESH,
            )
            for way, to in enumerate((right, left))
        ]

    def gather():
        return [
            pltpu.make_async_remote_copy(
                src_ref=sums[part], dst_ref=got3[k], send_sem=s3_send.at[k], recv_sem=s3_recv.at[k],
                device_id={"dp": to}, device_id_type=pl.DeviceIdType.MESH,
            )
            for k, (part, to) in enumerate(((0, right), (1, left), (1, right), (0, left)))
        ]

    def keep(p):
        slot = lax.rem(p, STAGES)
        return pltpu.make_async_copy(stage.at[slot, :, pl.ds(0, d)], mine.at[p], mine_sem.at[slot])

    def relay_loads(p):
        parts = mine.at[p, :, share(1, 0)], mine.at[p, :, share(3, 1)], got1.at[p, 0, :, upper_half], got1.at[p, 1, :, lower_half]
        return [pltpu.make_async_copy(part, rin.at[k], rin_sem.at[k]) for k, part in enumerate(parts)]

    def total_loads(p):
        parts = mine.at[p, :, share(0, 0)], mine.at[p, :, share(0, 1)], got2.at[p, 0], got2.at[p, 1]
        parts += got1.at[p, 1, :, upper_half], got1.at[p, 0, :, lower_half]
        return [pltpu.make_async_copy(part, tin.at[k], tin_sem.at[k]) for k, part in enumerate(parts)]

    def results(p, refs, at):
        slot = lax.rem(p, 2)
        return [pltpu.make_async_copy(tout.at[slot, part], ref.at[at], out_sem.at[slot, part]) for part, ref in enumerate(refs)]

    def when(p, body):
        @pl.when((p >= 0) & (p < pieces))
        def _():
            body(p)

    def settle(p):
        for copy in results(p, sums[:2], 0):
            copy.wait()

    def sent(copies):
        for copy in copies:
            copy.wait_send()

    def begin_relay(p):
        for copy in first(p):
            copy.wait_recv()
        for copy in relay_loads(p):
            copy.start()

    def begin_total(p):
        for copy in second(p):
            copy.wait_recv()
        for copy in total_loads(p):
            copy.start()

    def end_relay(p):
        for copy in relay_loads(p):
            copy.wait()
        when(p - RELAYS, lambda p: sent(second(p)))
        for way in range(2):
            rout[lax.rem(p, RELAYS), way] = (rin[way].astype(F32) + rin[2 + way].astype(F32)).astype(BF)
        for copy in second(p):
            copy.start()

    def end_total(p):
        for copy in total_loads(p):
            copy.wait()
        when(p - 2, settle)
        for part in range(2):
            value = tin[part].astype(F32) + tin[2 + part].astype(F32) + tin[4 + part].astype(F32)
            tout[lax.rem(p, 2), part] = value.astype(BF)
        for g, (start, size) in enumerate(groups):

            @pl.when((p >= start) & (p < start + size))
            def _():
                for copy in results(p, sums[2 * g : 2 * g + 2], p - start):
                    copy.start()

    def put(p):
        when(p - STAGES, lambda p: sent(first(p)))
        slot = lax.rem(p, STAGES)
        by_both = dot(at_ref[upper], both[lax.rem(p, 2)])
        for i, value in enumerate((by_both[:, :width], by_both[:, width:], dot(dyt[...], hid[...]))):
            value = value.astype(BF)
            stage[slot, i, :d] = value
            stage[slot, i, d:] = value[:half]
        keep(p).start()

    def forward(begin, final):
        def trip(j, _):
            hiddens = []
            for b in range(PAIR):
                i = j * PAIR + b
                rows = rows_of(i)
                if begin:
                    if b:
                        loads(i).wait()
                    else:
                        pl.when(i > 0)(lambda i=i: loads(i).wait())
                    a_ref[0, rows, :] = normed(xh[rows, :])
                a = a_ref[0, rows, :]
                for wg, wu in ((wg_ref, wu_ref), (wg2_ref, wu2_ref)):
                    gate = dot(a, wg[0])
                    up = dot(a, wu[0])
                    hiddens.append((gate * jax.nn.sigmoid(gate) * up).astype(BF))
            for b in range(PAIR):
                rows = rows_of(j * PAIR + b)
                part = dot(hiddens[2 * b], wd_ref[0]) + dot(hiddens[2 * b + 1], wd2_ref[0])
                if not begin:
                    part = total[rows, :] + part
                if not final:
                    total[rows, :] = part
                else:
                    total[rows, :] = jnp.zeros_like(part)
                    h = (xh[rows, :].astype(F32) + part.astype(BF).astype(F32)).astype(BF)
                    xh[rows, :] = h
                    a = normed(h)
                    a_ref[1, rows, :] = a
                    at_ref[1, :, rows] = a.T
            if not begin and not final:
                count = (steps - 2) * trips
                chunk = -(-t // count // LANES) * LANES
                at = lax.min(((s - 1) * trips + j) * (chunk // LANES), (t - chunk) // LANES) * LANES
                rows = pl.ds(pl.multiple_of(at, LANES), chunk)
                at_ref[0, :, rows] = a_ref[0, rows, :].T
                dyt[:, rows] = dy[rows, :].T
            return 0

        lax.fori_loop(0, trips, trip, 0)

    @pl.when(s == 0)
    def _():
        barrier = pltpu.get_barrier_semaphore()
        for to in (right, left):
            pl.semaphore_signal(barrier, inc=1, device_id={"dp": to}, device_id_type=pl.DeviceIdType.MESH)
        for i in range(1, t // ROWS):
            loads(i).start()
        dy_load.start()
        xh[rows_of(0), :] = x_ref[...]
        forward(True, False)
        pl.semaphore_wait(barrier, 2)

    pl.when(s == 1)(dy_load.wait)
    pl.when((s > 0) & (s < steps - 1))(lambda: forward(False, False))

    @pl.when(s == steps - 1)
    def _():
        forward(False, True)

    def begin():
        when(before, lambda p: keep(p).wait())
        when(relay_p, begin_relay)
        when(total_p, begin_total)

    @pl.when(computes)
    def _():
        slot = lax.rem(q, 2)
        pl.when((upper == 1) & (q >= 2))(lambda: save(q - 2).wait())
        for i in range(t // ROWS):
            rows = rows_of(i)
            x, g = a_ref[upper, rows, :], dy[rows, :]
            gate = dot(x, wg_ref[0])
            up = dot(x, wu_ref[0])
            dh = dot(g, wd_ref[0], 1, 1).astype(BF).astype(F32)
            sig = jax.nn.sigmoid(gate)
            act = gate * sig
            hid[rows, :] = (act * up).astype(BF)
            both[slot, rows, :width] = (dh * up * (sig * (1 + gate * (1 - sig)))).astype(BF)
            both[slot, rows, width:] = (dh * act).astype(BF)
        begin()
        put(q)
        pl.when(q < n - 2)(lambda: save(q).start())

    def by_inputs(i):
        rows, slot = rows_of(i), lax.rem(j, 2)
        return total[rows, :] + dot(both[slot, rows, :width], wg_ref[0], 1, 1) + dot(both[slot, rows, width:], wu_ref[0], 1, 1)

    @pl.when(inward)
    def _():
        begin()
        pl.when(j >= 2)(lambda: fetch(j - 2).wait())

    @pl.when(inward & (j < n - 1))
    def _():
        for i in range(t // ROWS):
            total[rows_of(i), :] = by_inputs(i)
        pl.when(j < n - 2)(lambda: fetch(j).start())

    @pl.when(j == n - 1)
    def _():
        for i in range(t // ROWS):
            rows = rows_of(i)
            da = by_inputs(i).astype(BF).astype(F32)
            h = xh[rows, :].astype(F32)
            scale = lax.rsqrt(jnp.mean(h**2, -1, keepdims=True) + 1e-6)
            inner = jnp.mean(da * h, -1, keepdims=True)
            by_h = da * scale - h * (inner * scale * scale * scale)
            g = (dy[rows, :].astype(F32) + by_h.astype(BF).astype(F32)).astype(BF)
            dy[rows, :] = g
            dyt[:, rows] = g.T

    pl.when(j >= 2 * n)(begin)
    when(relay_p, end_relay)
    when(total_p, end_total)

    @pl.when(relay_p == pieces - 1)
    def _():
        for copy in gather():
            copy.start()

    @pl.when(computes)
    def _():
        for copy in first(q):
            copy.start()

    @pl.when(s == pl.num_programs(0) - 1)
    def _():
        for p in range(pieces - STAGES, pieces):
            sent(first(p))
        for p in range(pieces - RELAYS, pieces):
            sent(second(p))
        for p in range(pieces - 2, pieces):
            settle(p)
        for copy in gather():
            copy.wait()


def reduced(ways, groups, width, x, dy, wg, wu, wd):
    t, d = x.shape
    layers, _, ff = wg.shape
    n, half = ff // width, d // ways // 2
    pieces = layers * n
    part = (3, half, width)
    steps = n // 2
    start = steps + 2 * n
    at = lambda s, first, upper, inward, lower: jnp.where(
        s < steps, first, jnp.where(s < steps + n, upper, jnp.where(s < start, inward, jnp.where(s < start + n, lower, n - 1)))
    )
    layer = lambda s: at(s, 0, 1, 1, 0) * (s < start)
    order = lambda s: lax.rem(s - steps + n - 2, n)
    col = pl.BlockSpec((1, d, width), lambda s: (layer(s), 0, at(s, 2 * s, s - steps, order(s), s - start)))
    row = pl.BlockSpec((1, width, d), lambda s: (layer(s), at(s, 2 * s, s - steps, n - 1, s - start), 0))
    other = lambda s: at(s, 2 * s + 1, n - 1, n - 1, n - 1)
    col2 = pl.BlockSpec((1, d, width), lambda s: (0, 0, other(s)))
    row2 = pl.BlockSpec((1, width, d), lambda s: (0, other(s), 0))
    dma = pltpu.SemaphoreType.DMA
    outs = [(size, *part) for _, size in groups for _ in range(2)] + [(pieces, 2, 3, 2 * half, width), (pieces, 2, *part), (pieces, 3, d, width), (n, t, 2 * width)]
    outs += [(groups[0][1], *part)] * 4
    got = pl.pallas_call(
        functools.partial(step_body, ways, groups),
        grid=(steps + 4 * n,),
        in_specs=[ANY, pl.BlockSpec((ROWS, d), lambda s: (0, 0)), ANY, col, col, row, col2, col2, row2],
        out_specs=[ANY] * len(outs),
        out_shape=[jax.ShapeDtypeStruct(o, BF) for o in outs],
        scratch_shapes=[
            pltpu.VMEM((t, d), BF), pltpu.VMEM((2, t, d), BF), pltpu.VMEM((t, d), BF), pltpu.VMEM((t, d), F32),
            pltpu.VMEM((2, d, t), BF), pltpu.VMEM((d, t), BF), pltpu.VMEM((2, t, 2 * width), BF), pltpu.VMEM((t, width), BF),
            pltpu.VMEM((STAGES, 3, d + half, width), BF), pltpu.VMEM((4, *part), BF), pltpu.VMEM((RELAYS, 2, *part), BF),
            pltpu.VMEM((6, *part), BF), pltpu.VMEM((2, 2, *part), BF),
            dma((t // ROWS,)), dma, dma((STAGES,)), dma((4,)), dma((6,)), dma((2, 2)),
            dma((2, pieces)), dma((2, pieces)), dma((2, pieces)), dma((2, pieces)), dma((4,)), dma((4,)), dma((2,)),
        ],
        compiler_params=pltpu.CompilerParams(vmem_limit_bytes=67_043_328, collective_id=0, has_side_effects=True),
        name="reduced",
    )(x, x, dy, wg, wu, wd, wg, wu, wd)
    return [got[2 * g : 2 * g + 2] for g in range(len(groups))], got[-4:]


SHARES = 7


def adamw(w, m, v, g):
    m = 0.9 * m + 0.1 * g
    v = 0.95 * v + 0.05 * g * g
    step = m * lax.rsqrt(v + 1e-8) + 0.1 * w
    return (w - 0.02 * step).astype(BF), m, v


def update_body(ways, steps, me_ref, *refs):
    parts, refs = refs[: 2 * ways], refs[2 * ways :]
    w, m, v = refs[0:3], refs[3:6], refs[6:9]
    outs, g_ref = refs[-10:-1], refs[-1]
    s = lax.rem(pl.program_id(0), steps)
    half = parts[0].shape[2]

    @pl.when(s == 0)
    def _():
        for k, ref in enumerate(parts):
            rows = aligned(lax.rem(me_ref[0] + k // 2, ways) * 2 + k % 2, half)
            for i in range(3):
                g_ref[i, rows, :] = ref[0, i]

    def apply(i, rows, g):
        results = adamw(w[i][0, rows, :].astype(F32), m[i][0, rows, :], v[i][0, rows, :], g)
        for out, value in zip(outs[i::3], results, strict=True):
            out[0, rows, :] = value

    now = w[0].shape[1]
    chunk = now // SHARES

    def trip(j, _):
        rows = aligned(j, chunk)
        for i in range(2):
            apply(i, rows, g_ref[i, aligned(s * SHARES + j, chunk), :].astype(F32))
        return 0

    lax.fori_loop(0, SHARES, trip, 0)
    apply(2, pl.ds(0, LANES), g_ref[2, :, aligned(s, LANES)].astype(F32).T)


def update(me, ways, number, start, parts, w, m, v, before):
    size, _, _, width = parts[0].shape
    d = w[0].shape[1]
    steps = width // LANES
    up = pl.BlockSpec((1, d // steps, width), lambda i, me: (number, lax.rem(i, steps), start + i // steps))
    down = pl.BlockSpec((1, LANES, d), lambda i, me: (number, start * steps + i, 0))
    some = pl.BlockSpec((1, *parts[0].shape[1:]), lambda i, me: (i // steps, 0, 0, 0))
    fill = list(before) if before is not None else []
    return pl.pallas_call(
        functools.partial(update_body, ways, steps),
        grid_spec=pltpu.PrefetchScalarGridSpec(
            num_scalar_prefetch=1,
            grid=(size * steps,),
            in_specs=[some] * len(parts) + [up, up, down] * 3 + [ANY] * len(fill),
            out_specs=[up, up, down] * 3,
            scratch_shapes=[pltpu.VMEM((3, d, width), BF)],
        ),
        out_shape=[jax.ShapeDtypeStruct(x.shape, dtype) for dtype in (BF, F32, F32) for x in w],
        input_output_aliases={1 + len(parts) + 9 + i: i for i in range(len(fill))},
        compiler_params=params(),
        name="update",
    )(me, *parts, *w, *m, *v, *fill)


WIDTH = 256
GROUPS = (4, 6, 3, 3, 2, 2)
ORDER = ("F0", "A1", "B1", "W0", "F1", "A3", "A4", "A2", "B2", "W1", "F2", "B3", "F3", "B4", "A5", "W2", "F4", "B5", "W3", "F5", "W4", "W5")


def solution(mesh):
    ways = mesh.shape["dp"]
    assert ways == 4
    rightward = [(i, (i + 1) % ways) for i in range(ways)]
    leftward = [(i, (i - 1) % ways) for i in range(ways)]

    def whole_step(x, dy, *arrays):
        w, m, v = (arrays[i : i + 3] for i in (0, 3, 6))
        layers, _, ff = w[0].shape
        n = ff // WIDTH
        assert layers == 2 and sum(GROUPS) == layers * n
        me = lax.axis_index("dp").astype(jnp.int32).reshape(1)
        groups = [(sum(GROUPS[:i]), size) for i, size in enumerate(GROUPS)]
        own, near = reduced(ways, groups, WIDTH, x[0], dy[0], *w)
        got, out = {("A", 0): (near[0], near[1]), ("B", 0): (near[3], near[2])}, None
        for op in ORDER:
            kind, g = op[0], int(op[1:])
            if kind == "W":
                (la, rb), (ra, lb), (fa, fb) = (got[k, g] for k in "ABF")
                start = groups[g][0]
                out = update(me, ways, layers - 1 - start // n, start % n, [*own[g], ra, rb, fa, fb, la, lb], w, m, v, out)
                continue
            right, left = {"A": own[g], "B": own[g][::-1], "F": got.get(("A", g))}[kind]
            right = lax.ppermute(right, "dp", rightward)
            left = lax.ppermute(left, "dp", leftward)
            got[kind, g] = (right, left) if kind != "B" else (left, right)
        return tuple(out)

    return jax.shard_map(
        whole_step,
        mesh=mesh,
        in_specs=(P(("rep", "dp"), None, None),) * 2 + (P(None, None, None),) * 9,
        out_specs=(P("rep", None, None),) * 9,
        check_vma=False,
    )
```
